32 devices in a mesh: tenant: 2 (over y), ctx: 2 (over x), head: 8 (over z, core).
Axes of the slice: x: 2, y: 2, z: 4, core: 2. Of those that a mesh axis runs over, the one named last changes fastest.
Arguments:
- tokens: bfloat16 [1024, 4608], P(('tenant', 'ctx'), 'head'), parts along dimension 0, may hold values from -6 to 6
- query_frozen_matrix: bfloat16 [4608, 2048], P('ctx', 'head'), may hold values from -0.09375 to 0.09375
- key_weight: bfloat16 [4608, 1024], P('ctx', 'head'), may hold values from -0.09375 to 0.09375
- value_frozen_matrix: bfloat16 [4608, 1024], P('ctx', 'head'), may hold values from -0.09375 to 0.09375
- query_down: bfloat16 [9216, 16], P('tenant'), parts along dimension 0, may hold values from -0.09375 to 0.09375
- query_adapter_expand: bfloat16 [32, 2048], P('tenant', 'head'), parts along dimension 0, may hold values from -1.5 to 1.5
- value_down: bfloat16 [9216, 16], P('tenant'), parts along dimension 0, may hold values from -0.09375 to 0.09375
- value_adapter_expand: bfloat16 [32, 1024], P('tenant', 'head'), parts along dimension 0, may hold values from -1.5 to 1.5
- block_order: int32 [8], P('tenant'), parts along dimension 0, may hold values from 0 to 3, each once
- doc_starts: int32 [24], P('tenant'), parts along dimension 0, may hold values from 0 to 511, as said below
- prompt_of: int32 [24], P('tenant'), parts along dimension 0, may hold values from 0 to 11, as said below
Outputs:
- attended: bfloat16 [1024, 2048], P(('tenant', 'ctx'), 'head'), parts along dimension 0
The draws below stay inside these ranges and needn't reach their ends.
There are 2 independent parts, one for each index of `tenant`. The reference program is written for one: setup_inputs(seed, part) draws one part's arguments, and reference() takes and returns one part's arrays. A program takes and returns all parts, laid end to end along the dimension named above; an argument that names none is the same for every part. Nothing has to cross between parts.
Inputs may be any that keep to these rules, and one draw needn't show every extreme that they name: `doc_starts`: strictly increasing with first entry 0; the segments come in 4 groups of three: a prompt, a chosen and a rejected response. `prompt_of`: for segment j = 3k it is j; for j = 3k + 1 it is 3k; for j = 3k + 2 it is 3k or j. `block_order`: each of 0 to 3 once.
All inputs are finite; a program needn't handle non-finite values.
Results may differ from the reference program's by a relative error of at most 0.012.
Values may be sent and summed in bfloat16 or wider, within the bound.
No kernel may reach another device: no remote copies, remote signals or barrier semaphores. Data moves between devices by JAX's collectives and lax.ppermute only.
A program may use at most 64 MiB of HBM per device.

```python
import math
import jax
import jax.numpy as jnp
from jax import lax

D = 4608
HEADS = 16
KV_HEADS = 8
HD = 128
RANK = 16
PAIRS = 4
TOK_DEV = 256
TOKENS = 512
SEGS = 12
BLOCKS = 4
N_CTX = 2


def draw_doc_starts(key, part):
    cuts = jax.random.permutation(jax.random.fold_in(key, 11), TOKENS - 1)[:SEGS - 1] + 1
    return jnp.concatenate([jnp.zeros((1,), jnp.int32), jnp.sort(cuts.astype(jnp.int32))])


def draw_prompt_of(key, part):
    flags = jax.random.randint(jax.random.fold_in(key, 23), (PAIRS,), 0, 2)
    seg_ids = jnp.arange(SEGS, dtype=jnp.int32)
    leading = 3 * (seg_ids // 3)
    within = seg_ids % 3
    reads = (within == 1) | (within == 2) & (flags[seg_ids // 3] == 1)
    return jnp.where(reads, leading, seg_ids).astype(jnp.int32)


def block_levels(stream_key, shape, shards, smallest, top_value):
    level, own = 1.0, jax.random.fold_in(stream_key, 6)
    for dim, blocks in shards:
        steps = jnp.exp(jax.random.uniform(jax.random.fold_in(own, dim), (blocks,), jnp.float32, smallest / len(shards), top_value / len(shards)))
        level = level * jnp.repeat(steps, shape[dim] // blocks).reshape([-1 if axis == dim else 1 for axis in range(len(shape))])
    return level


def bell_draw(key, extent, width, reach, cuts=(), held_as=jnp.bfloat16):
    values = jax.random.normal(key, extent, jnp.float32) * width
    if len(cuts) > 0:
        values = block_levels(key, extent, cuts, -0.22, 0.18) * values
    return jnp.clip(values, min=-reach, max=reach).astype(held_as)


def setup_inputs(seed: int = 0, part: int = 0) -> dict:
    key_of = jax.random.split(jax.random.key(seed), 12)
    part_keys = jax.random.split(jax.random.fold_in(key_of[11], part), 12)
    tokens = bell_draw(part_keys[0], (TOKENS, D), 1.0, 6.0, ((0, 2), (1, 8)))
    query_frozen_matrix = bell_draw(key_of[1], (D, HEADS * HD), D ** -0.5, 0.09375, ((0, 2), (1, 8)))
    key_weight = bell_draw(key_of[2], (D, KV_HEADS * HD), D ** -0.5, 0.09375, ((0, 2), (1, 8)))
    value_frozen_matrix = bell_draw(key_of[3], (D, KV_HEADS * HD), D ** -0.5, 0.09375, ((0, 2), (1, 8)))
    query_down = bell_draw(part_keys[4], (D, RANK), D ** -0.5, 0.09375)
    query_adapter_expand = bell_draw(part_keys[5], (RANK, HEADS * HD), RANK ** -0.5, 1.5, ((1, 8),))
    value_down = bell_draw(part_keys[6], (D, RANK), D ** -0.5, 0.09375)
    value_adapter_expand = bell_draw(part_keys[7], (RANK, KV_HEADS * HD), RANK ** -0.5, 1.5, ((1, 8),))
    block_order = jax.random.permutation(part_keys[8], BLOCKS).astype(jnp.int32)
    doc_starts = draw_doc_starts(jax.random.fold_in(jax.random.fold_in(key_of[11], part), 71), part)
    prompt_of = draw_prompt_of(jax.random.fold_in(jax.random.fold_in(key_of[11], part), 71), part)
    return {"tokens": tokens, "query_frozen_matrix": query_frozen_matrix, "key_weight": key_weight, "value_frozen_matrix": value_frozen_matrix, "query_down": query_down, "query_adapter_expand": query_adapter_expand, "value_down": value_down, "value_adapter_expand": value_adapter_expand, "block_order": block_order, "doc_starts": doc_starts, "prompt_of": prompt_of}


softcap_limit = 50.0
query_scale = 144.0 ** -0.5
adapter_scaling = 2.0
rope_base = 10000.0


def row_meta(row_ids, block_order, doc_starts, prompt_of, block_len, sequence_len):
    block_count = block_order.shape[0]
    block_id = row_ids // block_len
    one_hot = block_id[:, None] == jnp.arange(block_count, dtype=jnp.int32)[None, :]
    ordered = jnp.sum(jnp.where(one_hot, block_order[None, :], 0), axis=1).astype(jnp.int32)
    places = ordered * block_len + row_ids % block_len
    segment = jnp.sum((doc_starts[None, :] <= places[:, None]).astype(jnp.int32), axis=1) - 1
    seg_ids = jnp.arange(doc_starts.shape[0], dtype=jnp.int32)
    selected = segment[:, None] == seg_ids[None, :]
    prompt_seg = jnp.sum(jnp.where(selected, prompt_of[None, :], 0), axis=1).astype(jnp.int32)
    own_start = jnp.sum(jnp.where(selected, doc_starts[None, :], 0), axis=1).astype(jnp.int32)
    next_starts = jnp.concatenate([doc_starts[1:], jnp.full((1,), sequence_len, jnp.int32)])
    prompt_sel = prompt_seg[:, None] == seg_ids[None, :]
    prompt_len = jnp.sum(jnp.where(prompt_sel, (next_starts - doc_starts)[None, :], 0), axis=1).astype(jnp.int32)
    rotary_pos = places - own_start + jnp.where(prompt_seg != segment, prompt_len, 0)
    return places, segment, prompt_seg, rotary_pos


def rotate(values_in, rotary_pos):
    width_half = values_in.shape[-1] // 2
    frequency = jnp.exp(jnp.arange(width_half, dtype=jnp.float32) * (-2.0 * math.log(rope_base) / values_in.shape[-1]))
    angles = rotary_pos.astype(jnp.float32)[:, None] * frequency[None, :]
    cosine = jnp.concatenate([jnp.cos(angles), jnp.cos(angles)], axis=-1)[:, None, :]
    sine_part = jnp.concatenate([jnp.sin(angles), jnp.sin(angles)], axis=-1)[:, None, :]
    rotated = jnp.concatenate([-values_in[..., width_half:], values_in[..., :width_half]], axis=-1)
    return values_in * cosine + rotated * sine_part


def visible_mask(query_info, key_info):
    same_doc = (key_info[1][None, :] == query_info[1][:, None]) & (key_info[0][None, :] <= query_info[0][:, None])
    from_prompt = (key_info[1][None, :] == query_info[2][:, None]) & (query_info[2] != query_info[1])[:, None]
    return same_doc | from_prompt


def reference(tokens, query_frozen_matrix, key_weight, value_frozen_matrix, query_down, query_adapter_expand, value_down, value_adapter_expand, block_order, doc_starts, prompt_of):
    row_ids = jnp.arange(TOKENS, dtype=jnp.int32)
    row_info = row_meta(row_ids, block_order, doc_starts, prompt_of, TOK_DEV // 2, TOKENS)
    query_adapter_hidden = jnp.dot(tokens, query_down, preferred_element_type=jnp.float32).astype(jnp.bfloat16)
    query_states = jnp.dot(tokens, query_frozen_matrix, preferred_element_type=jnp.float32) + adapter_scaling * jnp.dot(query_adapter_hidden, query_adapter_expand, preferred_element_type=jnp.float32)
    query_states = (rotate(query_states.reshape(TOKENS, HEADS, HD), row_info[3]) * query_scale).astype(jnp.bfloat16)
    key_proj = jnp.dot(tokens, key_weight, preferred_element_type=jnp.float32).reshape(TOKENS, KV_HEADS, HD)
    key_proj = rotate(key_proj, row_info[3]).astype(jnp.bfloat16)
    value_adapter_hidden = jnp.dot(tokens, value_down, preferred_element_type=jnp.float32).astype(jnp.bfloat16)
    value_projected = jnp.dot(tokens, value_frozen_matrix, preferred_element_type=jnp.float32) + adapter_scaling * jnp.dot(value_adapter_hidden, value_adapter_expand, preferred_element_type=jnp.float32)
    value_projected = value_projected.astype(jnp.bfloat16).reshape(TOKENS, KV_HEADS, HD)
    per_kv = HEADS // KV_HEADS
    key_wide = key_proj.astype(jnp.float32)
    value_wide = value_projected.astype(jnp.float32)
    query_blocks = query_states.astype(jnp.float32).reshape(N_CTX, TOK_DEV, KV_HEADS, per_kv, HD)
    info_blocks = tuple(entry.reshape(N_CTX, TOK_DEV) for entry in row_info[:3])

    def one_block(inputs):
        query_block, places, segment, prompt_seg = inputs
        visible = visible_mask((places, segment, prompt_seg), row_info)
        scores = jnp.einsum("tkgd,skd->kgts", query_block, key_wide)
        capped = softcap_limit * jnp.tanh(scores / softcap_limit)
        unnorm = jnp.where(visible[None, None], jnp.exp(capped), jnp.zeros_like(capped))
        denominator = jnp.sum(unnorm, axis=-1)
        rounded = lax.optimization_barrier(unnorm.astype(jnp.bfloat16)).astype(jnp.float32)
        numerator = jnp.einsum("kgts,skd->tkgd", rounded, value_wide)
        return (numerator / jnp.transpose(denominator, (2, 0, 1))[..., None]).astype(jnp.bfloat16)

    blocks_out = lax.map(one_block, (query_blocks,) + info_blocks)
    return blocks_out.reshape(TOKENS, HEADS * HD)
```

```python
import math

import jax
import jax.numpy as jnp
from jax import lax
from jax.experimental import pallas as pl
from jax.experimental.pallas import tpu as pltpu
from jax.sharding import PartitionSpec as P

HD = 128


softcap_limit = 50.0
query_scale = 144.0 ** (-0.5)
adapter_scaling = 2.0
rope_base = 10000.0


def row_meta(row_ids, block_order, doc_starts, prompt_of, block_len, sequence_len):
    block_count = block_order.shape[0]
    block_id = row_ids // block_len
    one_hot = block_id[:, None] == jnp.arange(block_count, dtype=jnp.int32)[None, :]
    ordered = jnp.sum(jnp.where(one_hot, block_order[None, :], 0), axis=1)
    places = ordered * block_len + row_ids % block_len
    segment = jnp.sum((doc_starts[None, :] <= places[:, None]).astype(jnp.int32), axis=1) - 1
    seg_ids = jnp.arange(doc_starts.shape[0], dtype=jnp.int32)
    selected = segment[:, None] == seg_ids[None, :]
    prompt_seg = jnp.sum(jnp.where(selected, prompt_of[None, :], 0), axis=1)
    own_start = jnp.sum(jnp.where(selected, doc_starts[None, :], 0), axis=1)
    next_starts = jnp.concatenate([doc_starts[1:], jnp.full((1,), sequence_len, jnp.int32)])
    prompt_sel = prompt_seg[:, None] == seg_ids[None, :]
    prompt_len = jnp.sum(jnp.where(prompt_sel, (next_starts - doc_starts)[None, :], 0), axis=1)
    rotary_pos = places - own_start + jnp.where(prompt_seg != segment, prompt_len, 0)
    return (places, segment, prompt_seg, rotary_pos)


def rotate(values_in, rotary_pos):
    width_half = values_in.shape[-1] // 2
    frequency = jnp.exp(
        jnp.arange(width_half, dtype=jnp.float32)
        * (-2.0 * math.log(rope_base) / values_in.shape[-1])
    )
    angles = rotary_pos.astype(jnp.float32)[:, None] * frequency[None, :]
    cosine = jnp.concatenate([jnp.cos(angles), jnp.cos(angles)], axis=-1)[:, None, :]
    sine_part = jnp.concatenate([jnp.sin(angles), jnp.sin(angles)], axis=-1)[:, None, :]
    rotated = jnp.concatenate([-values_in[..., width_half:], values_in[..., :width_half]], axis=-1)
    return values_in * cosine + rotated * sine_part


def visible_mask(query_info, key_info):
    same_doc = (key_info[1][None, :] == query_info[1][:, None]) & (
        key_info[0][None, :] <= query_info[0][:, None]
    )
    from_prompt = (key_info[1][None, :] == query_info[2][:, None]) & (
        query_info[2] != query_info[1]
    )[:, None]
    return same_doc | from_prompt


def local(
    tokens,
    query_frozen_matrix,
    key_weight,
    value_frozen_matrix,
    query_down,
    query_adapter_expand,
    value_down,
    value_adapter_expand,
    block_order,
    doc_starts,
    prompt_of,
):
    tok_rows = tokens.shape[0]
    cycle_size = lax.axis_size("ctx")
    device = lax.axis_index("ctx")
    sequence_len = tok_rows * cycle_size
    block_len = tok_rows // 2
    full_tokens = lax.all_gather(tokens, "head", axis=1, tiled=True)

    def add_rows(weight_part):
        return jnp.dot(full_tokens, weight_part, preferred_element_type=jnp.float32)

    frozen_query_output = add_rows(lax.all_gather(query_frozen_matrix, "ctx", axis=0, tiled=True))
    key_base = add_rows(lax.all_gather(key_weight, "ctx", axis=0, tiled=True))
    frozen_value_output = add_rows(lax.all_gather(value_frozen_matrix, "ctx", axis=0, tiled=True))
    own_ids = device * tok_rows + jnp.arange(tok_rows, dtype=jnp.int32)
    own_info = row_meta(own_ids, block_order, doc_starts, prompt_of, block_len, sequence_len)
    local_heads = query_frozen_matrix.shape[1] // HD
    local_kv = key_weight.shape[1] // HD
    per_kv = local_heads // local_kv
    query_adapter_hidden = jnp.dot(
        full_tokens, query_down, preferred_element_type=jnp.float32
    ).astype(jnp.bfloat16)
    query_states = frozen_query_output + adapter_scaling * jnp.dot(
        query_adapter_hidden, query_adapter_expand, preferred_element_type=jnp.float32
    )
    query_states = (
        rotate(query_states.reshape(tok_rows, local_heads, HD), own_info[3]) * query_scale
    ).astype(jnp.bfloat16)
    query_heads = query_states.reshape(tok_rows, local_kv, per_kv, HD)
    key_proj = (
        rotate(key_base.reshape(tok_rows, local_kv, HD), own_info[3])
        .astype(jnp.bfloat16)
        .reshape(tok_rows, local_kv * HD)
    )
    value_adapter_hidden = jnp.dot(
        full_tokens, value_down, preferred_element_type=jnp.float32
    ).astype(jnp.bfloat16)
    value_projected = (
        frozen_value_output
        + adapter_scaling
        * jnp.dot(value_adapter_hidden, value_adapter_expand, preferred_element_type=jnp.float32)
    ).astype(jnp.bfloat16)
    pieces = (
        lax.all_gather(key_proj, "ctx", axis=0, tiled=True),
        lax.all_gather(value_projected, "ctx", axis=0, tiled=True),
    )
    key_ids = jnp.arange(pieces[0].shape[0], dtype=jnp.int32)
    key_block = pieces[0]
    value_block = pieces[1]
    key_info = row_meta(key_ids, block_order, doc_starts, prompt_of, block_len, sequence_len)
    visible = visible_mask(own_info, key_info)
    key_heads = key_block.reshape(key_block.shape[0], local_kv, HD)
    value_heads = value_block.reshape(value_block.shape[0], local_kv, HD)
    scores = jnp.einsum(
        "tkgd,skd->kgts", query_heads, key_heads, preferred_element_type=jnp.float32
    )
    capped = softcap_limit * jnp.tanh(scores / softcap_limit)
    unnorm = jnp.where(visible[None, None], jnp.exp(capped), jnp.zeros_like(capped))
    denominator = jnp.sum(unnorm, axis=-1)
    numerator = jnp.einsum(
        "kgts,skd->tkgd",
        unnorm.astype(jnp.bfloat16),
        value_heads,
        preferred_element_type=jnp.float32,
    )
    numerator, denominator = (numerator, denominator)
    attended = numerator / jnp.transpose(denominator, (2, 0, 1))[..., None]
    return attended.reshape(tok_rows, local_heads * HD).astype(jnp.bfloat16)


VMEM = pl.BlockSpec(memory_space=pltpu.VMEM)
SMEM = pl.BlockSpec(memory_space=pltpu.SMEM)
F32, BF16 = jnp.float32, jnp.bfloat16


def call(body, outs, in_specs, flops, **kw):
    multi = isinstance(outs, (list, tuple))
    return pl.pallas_call(
        body,
        out_shape=outs,
        in_specs=in_specs,
        out_specs=[VMEM] * len(outs) if multi else VMEM,
        cost_estimate=pl.CostEstimate(flops=flops, bytes_accessed=1 << 20, transcendentals=0),
        compiler_params=pltpu.CompilerParams(vmem_limit_bytes=12 << 20),
        **kw,
    )


def prep_body(q_ref, k_ref, v_ref, dq_ref, dv_ref, out_ref):
    depth = out_ref.shape[2]
    for b in range(out_ref.shape[0]):
        at = 0
        span = slice(b * depth, (b + 1) * depth)
        for ref in (q_ref, k_ref, v_ref):
            out_ref[b, at : at + ref.shape[1], :] = ref[span, :].T
            at += ref.shape[1]
        for ref in (dq_ref, dv_ref):
            out_ref[b, at : at + ref.shape[0], :] = ref[:, span]
            at += ref.shape[0]


def dot(a, b):
    return jnp.dot(a, b, preferred_element_type=F32)


def first_body(ids_ref, w_ref, m0, m1, n0, n1, out_m, out_n):
    own, twin = ids_ref[0], ids_ref[1]
    out_m[...] = dot(w_ref[own], m0[...]) + dot(w_ref[twin], m1[...])
    out_n[...] = dot(w_ref[own], n0[...]) + dot(w_ref[twin], n1[...])


def second_body(wide_q, first_sent, ids_ref, w_ref, x0, x1, part, eq_ref, ev_ref, keep, send):
    own, twin = ids_ref[2], ids_ref[3]
    total = part[...] + dot(w_ref[own], x0[...]) + dot(w_ref[twin], x1[...])
    rank = eq_ref.shape[1]
    wide_v = ev_ref.shape[0]
    wide = send.shape[0] + first_sent
    low_q = total[wide : wide + rank].astype(BF16)
    low_v = total[wide + rank : wide + 2 * rank].astype(BF16)
    query = total[:wide_q] + dot(eq_ref[...], low_q)
    key = total[wide_q : wide - wide_v]
    value = total[wide - wide_v : wide] + dot(ev_ref[...], low_v)
    keep[:wide_q] = query
    keep[wide_q : wide - wide_v] = key
    keep[wide - wide_v :] = value
    if first_sent == 0:
        send[:wide_q] = query.astype(BF16)
    send[wide_q - first_sent : wide - wide_v - first_sent] = key.astype(BF16)
    send[wide - wide_v - first_sent :] = value.astype(BF16)


def turn(x, cos, sin):
    half = x.shape[0] // 2
    a, b = x[:half], x[half:]
    return jnp.concatenate([a * cos - b * sin, b * cos + a * sin], axis=0)


def attend_body(heads, mine, mine_in, other, other_in, cos_ref, sin_ref, vis_ref, out_ref):
    rows = mine.shape[1]
    wide_q = heads * HD
    cos, sin = cos_ref[...], sin_ref[...]
    cos_n, sin_n = cos[:, :rows], sin[:, :rows]
    total = mine[...] + mine_in[...].astype(F32)
    queries = jnp.concatenate(
        [
            (turn(total[h * HD : (h + 1) * HD], cos_n, sin_n) * query_scale).astype(BF16)
            for h in range(heads)
        ],
        axis=1,
    )
    rest = other[wide_q:] + other_in[...].astype(F32)
    keys = jnp.concatenate([total[wide_q : wide_q + HD], rest[:HD]], axis=1)
    keys = turn(keys, cos, sin).astype(BF16)
    values = jnp.concatenate(
        [total[wide_q + HD :].astype(BF16), rest[HD:].astype(BF16)], axis=1
    )
    scores = dot(keys.T, queries)
    capped = softcap_limit * jnp.tanh(scores / softcap_limit)
    weights = jnp.exp(capped)
    visible = vis_ref[...]
    for h in range(heads):
        w = weights[:, h * rows : (h + 1) * rows] * visible
        denominator = jnp.sum(w, axis=0, keepdims=True)
        numerator = dot(values, w.astype(BF16))
        out_ref[:, h * HD : (h + 1) * HD] = (numerator / denominator).T.astype(BF16)


def local_fast(
    tokens,
    query_frozen_matrix,
    key_weight,
    value_frozen_matrix,
    query_down,
    query_adapter_expand,
    value_down,
    value_adapter_expand,
    block_order,
    doc_starts,
    prompt_of,
):
    rows, depth = tokens.shape
    c, h = lax.axis_index("ctx"), lax.axis_index("head")
    chips = lax.axis_size("head") // 2
    sequence_len = rows * 2
    z = h // 2
    near = (z // 2) == c
    both = ("ctx", "head")

    def at(ci, zi, k):
        return ci * chips * 2 + zi * 2 + k

    q1_pairs, q2_pairs, z_pairs, zf_pairs = [], [], [], []
    for ci in range(2):
        for zi in range(chips):
            for k in range(2):
                me = at(ci, zi, k)
                z_pairs.append((me, at(ci, zi ^ 1, k)))
                if zi // 2 == ci:
                    q1_pairs.append((me, at(ci, zi ^ 2, k)))
                    q2_pairs.append((me, at(ci, zi ^ 1, k)))
                else:
                    q1_pairs.append((me, at(1 - ci, zi, k)))
                    q2_pairs.append((me, at(1 - ci, zi ^ 2, k)))
                    zf_pairs.append((me, at(ci, zi ^ 1, k)))
    core = [(i, i ^ 1) for i in range(chips * 2)]

    def send(x, pairs):
        return lax.ppermute(x, both, pairs)

    def twin(x):
        return lax.ppermute(x, "head", core)

    own = tokens.T
    q1 = send(own, q1_pairs)
    q2 = send(own, q2_pairs)
    other_a = jnp.where(near, q1, q2)
    mine_a = jnp.where(near, own, q1)
    other_b = send(other_a, z_pairs)
    late = send(q1, zf_pairs)
    mine_b = jnp.where(near, q2, late)

    own_ids = c * rows + jnp.arange(rows, dtype=jnp.int32)
    key_ids = jnp.concatenate([own_ids, (1 - c) * rows + jnp.arange(rows, dtype=jnp.int32)])
    info = lambda ids: row_meta(ids, block_order, doc_starts, prompt_of, rows // 2, sequence_len)
    own_info, key_info = info(own_ids), info(key_ids)
    visible = visible_mask(own_info, key_info).T.astype(F32)
    frequency = jnp.exp(
        jnp.arange(HD // 2, dtype=F32) * (-2.0 * math.log(rope_base) / HD)
    )
    angles = frequency[:, None] * key_info[3].astype(F32)[None, :]
    cos, sin = jnp.cos(angles), jnp.sin(angles)

    wide_q, wide_kv = query_frozen_matrix.shape[1], key_weight.shape[1]
    wide = wide_q + 2 * wide_kv
    rank = query_down.shape[1]
    half = query_frozen_matrix.shape[0]
    parts = half // depth
    down_q = lax.dynamic_slice_in_dim(query_down.T, c * half, half, axis=1)
    down_v = lax.dynamic_slice_in_dim(value_down.T, c * half, half, axis=1)
    expand_q = (adapter_scaling * query_adapter_expand).astype(BF16).T
    expand_v = (adapter_scaling * value_adapter_expand).astype(BF16).T
    weights = call(
        prep_body,
        jax.ShapeDtypeStruct((parts, wide + 2 * rank, depth), BF16),
        [VMEM] * 5,
        10**9,
    )(query_frozen_matrix, key_weight, value_frozen_matrix, down_q, down_v)

    k = h % 2
    par = (z % 2) * 2
    ids = jnp.stack([par + k, par + 1 - k, 2 - par + k, 3 - par - k]).astype(jnp.int32)

    whole = jax.ShapeDtypeStruct((wide + 2 * rank, rows), F32)
    kept = jax.ShapeDtypeStruct((wide, rows), F32)
    part_m, part_n = call(first_body, [whole, whole], [SMEM] + [VMEM] * 5, 10**9)(
        ids, weights, other_a, twin(other_a), mine_a, twin(mine_a)
    )

    def second(first_sent):
        def body(*refs):
            second_body(wide_q, first_sent, *refs)

        outs = [kept, jax.ShapeDtypeStruct((wide - first_sent, rows), BF16)]
        return call(body, outs, [SMEM] + [VMEM] * 6, 5 * 10**8)

    other_keep, other_send = second(0)(
        ids, weights, other_b, twin(other_b), part_m, expand_q, expand_v
    )
    swap = [(0, 1), (1, 0)]
    mine_in = lax.ppermute(other_send, "ctx", swap)
    mine_keep, mine_send = second(wide_q)(
        ids, weights, mine_b, twin(mine_b), part_n, expand_q, expand_v
    )
    other_in = lax.ppermute(mine_send, "ctx", swap)

    heads = wide_q // HD

    def last(*refs):
        attend_body(heads, *refs)

    return call(last, jax.ShapeDtypeStruct((rows, wide_q), BF16), [VMEM] * 7, 10**9)(
        mine_keep, mine_in, other_keep, other_in, cos, sin, visible
    )


def solution(mesh):
    in_specs = (
        P(("tenant", "ctx"), "head"),
        P("ctx", "head"),
        P("ctx", "head"),
        P("ctx", "head"),
        P("tenant", None),
        P("tenant", "head"),
        P("tenant", None),
        P("tenant", "head"),
        P("tenant"),
        P("tenant"),
        P("tenant"),
    )
    out_specs = P(("tenant", "ctx"), "head")
    fits = mesh.shape["ctx"] == 2 and mesh.shape["head"] == 8
    body = local_fast if fits else local
    return jax.shard_map(body, mesh=mesh, in_specs=in_specs, out_specs=out_specs, check_vma=False)
```

```python
import math

import jax
import jax.numpy as jnp
from jax import lax
from jax.experimental import pallas as pl
from jax.experimental.pallas import tpu as pltpu
from jax.sharding import PartitionSpec as P


HD = 128


softcap_limit = 50.0
query_scale = 144.0 ** (-0.5)
adapter_scaling = 2.0
rope_base = 10000.0


def row_meta(row_ids, block_order, doc_starts, prompt_of, block_len, sequence_len):
    block_count = block_order.shape[0]
    block_id = row_ids // block_len
    one_hot = block_id[:, None] == jnp.arange(block_count, dtype=jnp.int32)[None, :]
    ordered = jnp.sum(jnp.where(one_hot, block_order[None, :], 0), axis=1)
    places = ordered * block_len + row_ids % block_len
    segment = jnp.sum((doc_starts[None, :] <= places[:, None]).astype(jnp.int32), axis=1) - 1
    seg_ids = jnp.arange(doc_starts.shape[0], dtype=jnp.int32)
    selected = segment[:, None] == seg_ids[None, :]
    prompt_seg = jnp.sum(jnp.where(selected, prompt_of[None, :], 0), axis=1)
    own_start = jnp.sum(jnp.where(selected, doc_starts[None, :], 0), axis=1)
    next_starts = jnp.concatenate([doc_starts[1:], jnp.full((1,), sequence_len, jnp.int32)])
    prompt_sel = prompt_seg[:, None] == seg_ids[None, :]
    prompt_len = jnp.sum(jnp.where(prompt_sel, (next_starts - doc_starts)[None, :], 0), axis=1)
    rotary_pos = places - own_start + jnp.where(prompt_seg != segment, prompt_len, 0)
    return (places, segment, prompt_seg, rotary_pos)


def rotate(values_in, rotary_pos):
    width_half = values_in.shape[-1] // 2
    frequency = jnp.exp(
        jnp.arange(width_half, dtype=jnp.float32)
        * (-2.0 * math.log(rope_base) / values_in.shape[-1])
    )
    angles = rotary_pos.astype(jnp.float32)[:, None] * frequency[None, :]
    cosine = jnp.concatenate([jnp.cos(angles), jnp.cos(angles)], axis=-1)[:, None, :]
    sine_part = jnp.concatenate([jnp.sin(angles), jnp.sin(angles)], axis=-1)[:, None, :]
    rotated = jnp.concatenate([-values_in[..., width_half:], values_in[..., :width_half]], axis=-1)
    return values_in * cosine + rotated * sine_part


def visible_mask(query_info, key_info):
    same_doc = (key_info[1][None, :] == query_info[1][:, None]) & (
        key_info[0][None, :] <= query_info[0][:, None]
    )
    from_prompt = (key_info[1][None, :] == query_info[2][:, None]) & (
        query_info[2] != query_info[1]
    )[:, None]
    return same_doc | from_prompt


def local(
    tokens,
    query_frozen_matrix,
    key_weight,
    value_frozen_matrix,
    query_down,
    query_adapter_expand,
    value_down,
    value_adapter_expand,
    block_order,
    doc_starts,
    prompt_of,
):
    tok_rows = tokens.shape[0]
    cycle_size = lax.axis_size("ctx")
    device = lax.axis_index("ctx")
    sequence_len = tok_rows * cycle_size
    block_len = tok_rows // 2
    full_tokens = lax.all_gather(tokens, "head", axis=1, tiled=True)

    def add_rows(weight_part):
        return jnp.dot(full_tokens, weight_part, preferred_element_type=jnp.float32)

    frozen_query_output = add_rows(lax.all_gather(query_frozen_matrix, "ctx", axis=0, tiled=True))
    key_base = add_rows(lax.all_gather(key_weight, "ctx", axis=0, tiled=True))
    frozen_value_output = add_rows(lax.all_gather(value_frozen_matrix, "ctx", axis=0, tiled=True))
    own_ids = device * tok_rows + jnp.arange(tok_rows, dtype=jnp.int32)
    own_info = row_meta(own_ids, block_order, doc_starts, prompt_of, block_len, sequence_len)
    local_heads = query_frozen_matrix.shape[1] // HD
    local_kv = key_weight.shape[1] // HD
    per_kv = local_heads // local_kv
    query_adapter_hidden = jnp.dot(
        full_tokens, query_down, preferred_element_type=jnp.float32
    ).astype(jnp.bfloat16)
    query_states = frozen_query_output + adapter_scaling * jnp.dot(
        query_adapter_hidden, query_adapter_expand, preferred_element_type=jnp.float32
    )
    query_states = (
        rotate(query_states.reshape(tok_rows, local_heads, HD), own_info[3]) * query_scale
    ).astype(jnp.bfloat16)
    query_heads = query_states.reshape(tok_rows, local_kv, per_kv, HD)
    key_proj = (
        rotate(key_base.reshape(tok_rows, local_kv, HD), own_info[3])
        .astype(jnp.bfloat16)
        .reshape(tok_rows, local_kv * HD)
    )
    value_adapter_hidden = jnp.dot(
        full_tokens, value_down, preferred_element_type=jnp.float32
    ).astype(jnp.bfloat16)
    value_projected = (
        frozen_value_output
        + adapter_scaling
        * jnp.dot(value_adapter_hidden, value_adapter_expand, preferred_element_type=jnp.float32)
    ).astype(jnp.bfloat16)
    pieces = (
        lax.all_gather(key_proj, "ctx", axis=0, tiled=True),
        lax.all_gather(value_projected, "ctx", axis=0, tiled=True),
    )
    key_ids = jnp.arange(pieces[0].shape[0], dtype=jnp.int32)
    key_block = pieces[0]
    value_block = pieces[1]
    key_info = row_meta(key_ids, block_order, doc_starts, prompt_of, block_len, sequence_len)
    visible = visible_mask(own_info, key_info)
    key_heads = key_block.reshape(key_block.shape[0], local_kv, HD)
    value_heads = value_block.reshape(value_block.shape[0], local_kv, HD)
    scores = jnp.einsum(
        "tkgd,skd->kgts", query_heads, key_heads, preferred_element_type=jnp.float32
    )
    capped = softcap_limit * jnp.tanh(scores / softcap_limit)
    unnorm = jnp.where(visible[None, None], jnp.exp(capped), jnp.zeros_like(capped))
    denominator = jnp.sum(unnorm, axis=-1)
    numerator = jnp.einsum(
        "kgts,skd->tkgd",
        unnorm.astype(jnp.bfloat16),
        value_heads,
        preferred_element_type=jnp.float32,
    )
    numerator, denominator = (numerator, denominator)
    attended = numerator / jnp.transpose(denominator, (2, 0, 1))[..., None]
    return attended.reshape(tok_rows, local_heads * HD).astype(jnp.bfloat16)


VMEM = pl.BlockSpec(memory_space=pltpu.VMEM)
SMEM = pl.BlockSpec(memory_space=pltpu.SMEM)
F32, BF16 = jnp.float32, jnp.bfloat16


def call(body, outs, in_specs, flops, **kw):
    multi = isinstance(outs, (list, tuple))
    return pl.pallas_call(
        body,
        out_shape=outs,
        in_specs=in_specs,
        out_specs=[VMEM] * len(outs) if multi else VMEM,
        cost_estimate=pl.CostEstimate(flops=flops, bytes_accessed=1 << 20, transcendentals=0),
        compiler_params=pltpu.CompilerParams(vmem_limit_bytes=12 << 20),
        **kw,
    )


def prep_body(q_ref, k_ref, v_ref, dq_ref, dv_ref, out_ref):
    depth = out_ref.shape[2]
    for b in range(out_ref.shape[0]):
        at = 0
        span = slice(b * depth, (b + 1) * depth)
        for ref in (q_ref, k_ref, v_ref):
            out_ref[b, at : at + ref.shape[1], :] = ref[span, :].T
            at += ref.shape[1]
        for ref in (dq_ref, dv_ref):
            out_ref[b, at : at + ref.shape[0], :] = ref[:, span]
            at += ref.shape[0]


def dot(a, b):
    return jnp.dot(a, b, preferred_element_type=F32)


def first_body(ids_ref, w_ref, m0, m1, n0, n1, out_m, out_n):
    own, twin = ids_ref[0], ids_ref[1]
    out_m[...] = dot(w_ref[own], m0[...]) + dot(w_ref[twin], m1[...])
    out_n[...] = dot(w_ref[own], n0[...]) + dot(w_ref[twin], n1[...])


def second_body(wide_q, first_sent, ids_ref, w_ref, x0, x1, part, eq_ref, ev_ref, keep, send):
    own, twin = ids_ref[2], ids_ref[3]
    total = part[...] + dot(w_ref[own], x0[...]) + dot(w_ref[twin], x1[...])
    rank = eq_ref.shape[1]
    wide_v = ev_ref.shape[0]
    wide = send.shape[0] + first_sent
    low_q = total[wide : wide + rank].astype(BF16)
    low_v = total[wide + rank : wide + 2 * rank].astype(BF16)
    query = total[:wide_q] + dot(eq_ref[...], low_q)
    key = total[wide_q : wide - wide_v]
    value = total[wide - wide_v : wide] + dot(ev_ref[...], low_v)
    keep[:wide_q] = query
    keep[wide_q : wide - wide_v] = key
    keep[wide - wide_v :] = value
    if first_sent == 0:
        send[:wide_q] = query.astype(BF16)
    send[wide_q - first_sent : wide - wide_v - first_sent] = key.astype(BF16)
    send[wide - wide_v - first_sent :] = value.astype(BF16)


def pick_body(flag_ref, a_ref, b_ref, out_ref):
    @pl.when(flag_ref[0] == 1)
    def _():
        out_ref[...] = a_ref[...]

    @pl.when(flag_ref[0] != 1)
    def _():
        out_ref[...] = b_ref[...]


def turn(x, cos, sin):
    half = x.shape[0] // 2
    a, b = x[:half], x[half:]
    return jnp.concatenate([a * cos - b * sin, b * cos + a * sin], axis=0)


def attend_body(heads, mine, mine_in, other, other_in, cos_ref, sin_ref, vis_ref, out_ref):
    rows = mine.shape[1]
    wide_q = heads * HD
    cos, sin = cos_ref[...], sin_ref[...]
    cos_n, sin_n = cos[:, :rows], sin[:, :rows]
    total = mine[...] + mine_in[...].astype(F32)
    queries = jnp.concatenate(
        [
            (turn(total[h * HD : (h + 1) * HD], cos_n, sin_n) * query_scale).astype(BF16)
            for h in range(heads)
        ],
        axis=1,
    )
    rest = other[wide_q:] + other_in[...].astype(F32)
    keys = jnp.concatenate([total[wide_q : wide_q + HD], rest[:HD]], axis=1)
    keys = turn(keys, cos, sin).astype(BF16)
    values = jnp.concatenate(
        [total[wide_q + HD :].astype(BF16), rest[HD:].astype(BF16)], axis=1
    )
    scores = dot(keys.T, queries)
    capped = softcap_limit * jnp.tanh(scores / softcap_limit)
    weights = jnp.exp(capped)
    visible = vis_ref[...]
    for h in range(heads):
        w = weights[:, h * rows : (h + 1) * rows] * visible
        denominator = jnp.sum(w, axis=0, keepdims=True)
        numerator = dot(values, w.astype(BF16))
        out_ref[:, h * HD : (h + 1) * HD] = (numerator / denominator).T.astype(BF16)


def local_fast(
    tokens,
    query_frozen_matrix,
    key_weight,
    value_frozen_matrix,
    query_down,
    query_adapter_expand,
    value_down,
    value_adapter_expand,
    block_order,
    doc_starts,
    prompt_of,
):
    rows, depth = tokens.shape
    c, h = lax.axis_index("ctx"), lax.axis_index("head")
    chips = lax.axis_size("head") // 2
    sequence_len = rows * 2
    z = h // 2
    near = (z // 2) == c
    both = ("ctx", "head")

    def at(ci, zi, k):
        return ci * chips * 2 + zi * 2 + k

    q1_pairs, q2_pairs, z_pairs, zf_pairs = [], [], [], []
    for ci in range(2):
        for zi in range(chips):
            for k in range(2):
                me = at(ci, zi, k)
                z_pairs.append((me, at(ci, zi ^ 1, k)))
                if zi // 2 == ci:
                    q1_pairs.append((me, at(ci, zi ^ 2, k)))
                    q2_pairs.append((me, at(ci, zi ^ 1, k)))
                else:
                    q1_pairs.append((me, at(1 - ci, zi, k)))
                    q2_pairs.append((me, at(1 - ci, zi ^ 2, k)))
                    zf_pairs.append((me, at(ci, zi ^ 1, k)))
    core = [(i, i ^ 1) for i in range(chips * 2)]

    def send(x, pairs):
        return lax.ppermute(x, both, pairs)

    def twin(x):
        return lax.ppermute(x, "head", core)

    own = tokens.T
    q1 = send(own, q1_pairs)
    q2 = send(own, q2_pairs)

    own_ids = c * rows + jnp.arange(rows, dtype=jnp.int32)
    key_ids = jnp.concatenate([own_ids, (1 - c) * rows + jnp.arange(rows, dtype=jnp.int32)])
    info = lambda ids: row_meta(ids, block_order, doc_starts, prompt_of, rows // 2, sequence_len)
    own_info, key_info = info(own_ids), info(key_ids)
    visible = visible_mask(own_info, key_info).T.astype(F32)
    frequency = jnp.exp(
        jnp.arange(HD // 2, dtype=F32) * (-2.0 * math.log(rope_base) / HD)
    )
    angles = frequency[:, None] * key_info[3].astype(F32)[None, :]
    cos, sin = jnp.cos(angles), jnp.sin(angles)

    wide_q, wide_kv = query_frozen_matrix.shape[1], key_weight.shape[1]
    wide = wide_q + 2 * wide_kv
    rank = query_down.shape[1]
    half = query_frozen_matrix.shape[0]
    parts = half // depth
    down_q = lax.dynamic_slice_in_dim(query_down.T, c * half, half, axis=1)
    down_v = lax.dynamic_slice_in_dim(value_down.T, c * half, half, axis=1)
    expand_q = (adapter_scaling * query_adapter_expand).astype(BF16).T
    expand_v = (adapter_scaling * value_adapter_expand).astype(BF16).T
    weights = call(
        prep_body,
        jax.ShapeDtypeStruct((parts, wide + 2 * rank, depth), BF16),
        [VMEM] * 5,
        10**9,
    )(query_frozen_matrix, key_weight, value_frozen_matrix, down_q, down_v)

    k = h % 2
    par = (z % 2) * 2
    ids = jnp.stack([par + k, par + 1 - k, 2 - par + k, 3 - par - k]).astype(jnp.int32)

    whole = jax.ShapeDtypeStruct((wide + 2 * rank, rows), F32)
    kept = jax.ShapeDtypeStruct((wide, rows), F32)
    flag = near.astype(jnp.int32)[None]
    tables = (weights, ids, flag, expand_q, expand_v, visible)
    q1, q2, tables = lax.optimization_barrier((q1, q2, tables))
    weights, ids, flag, expand_q, expand_v, visible = tables

    def pick(a, b):
        out = jax.ShapeDtypeStruct(a.shape, a.dtype)
        return call(pick_body, out, [SMEM, VMEM, VMEM], 10**7)(flag, a, b)

    other_a = pick(q1, q2)
    other_b = send(other_a, z_pairs)
    late = send(q1, zf_pairs)
    mine_a = pick(own, q1)
    other_a_twin = twin(other_a)
    mine_a_twin = twin(mine_a)
    part_m, part_n = call(first_body, [whole, whole], [SMEM] + [VMEM] * 5, 10**9)(
        ids, weights, other_a, other_a_twin, mine_a, mine_a_twin
    )
    mine_b = pick(q2, late)

    def second(first_sent):
        def body(*refs):
            second_body(wide_q, first_sent, *refs)

        outs = [kept, jax.ShapeDtypeStruct((wide - first_sent, rows), BF16)]
        return call(body, outs, [SMEM] + [VMEM] * 6, 5 * 10**8)

    other_keep, other_send = second(0)(
        ids, weights, other_b, twin(other_b), part_m, expand_q, expand_v
    )
    swap = [(0, 1), (1, 0)]
    mine_in = lax.ppermute(other_send, "ctx", swap)
    mine_keep, mine_send = second(wide_q)(
        ids, weights, mine_b, twin(mine_b), part_n, expand_q, expand_v
    )
    other_in = lax.ppermute(mine_send, "ctx", swap)

    heads = wide_q // HD

    def last(*refs):
        attend_body(heads, *refs)

    return call(last, jax.ShapeDtypeStruct((rows, wide_q), BF16), [VMEM] * 7, 10**9)(
        mine_keep, mine_in, other_keep, other_in, cos, sin, visible
    )


def solution(mesh):
    in_specs = (
        P(("tenant", "ctx"), "head"),
        P("ctx", "head"),
        P("ctx", "head"),
        P("ctx", "head"),
        P("tenant", None),
        P("tenant", "head"),
        P("tenant", None),
        P("tenant", "head"),
        P("tenant"),
        P("tenant"),
        P("tenant"),
    )
    out_specs = P(("tenant", "ctx"), "head")
    fits = mesh.shape["ctx"] == 2 and mesh.shape["head"] == 8

    def body(*args):
        if not fits:
            return local(*args)
        return local_fast(*args)

    return jax.shard_map(
        body, mesh=mesh, in_specs=in_specs, out_specs=out_specs, check_vma=False
    )
```

```python
import math

import jax
import jax.numpy as jnp
from jax import lax
from jax.experimental import pallas as pl
from jax.experimental.pallas import tpu as pltpu
from jax.sharding import PartitionSpec as P


HD = 128


softcap_limit = 50.0
query_scale = 144.0 ** (-0.5)
adapter_scaling = 2.0
rope_base = 10000.0


def row_meta(row_ids, block_order, doc_starts, prompt_of, block_len, sequence_len):
    block_count = block_order.shape[0]
    block_id = row_ids // block_len
    one_hot = block_id[:, None] == jnp.arange(block_count, dtype=jnp.int32)[None, :]
    ordered = jnp.sum(jnp.where(one_hot, block_order[None, :], 0), axis=1)
    places = ordered * block_len + row_ids % block_len
    segment = jnp.sum((doc_starts[None, :] <= places[:, None]).astype(jnp.int32), axis=1) - 1
    seg_ids = jnp.arange(doc_starts.shape[0], dtype=jnp.int32)
    selected = segment[:, None] == seg_ids[None, :]
    prompt_seg = jnp.sum(jnp.where(selected, prompt_of[None, :], 0), axis=1)
    own_start = jnp.sum(jnp.where(selected, doc_starts[None, :], 0), axis=1)
    next_starts = jnp.concatenate([doc_starts[1:], jnp.full((1,), sequence_len, jnp.int32)])
    prompt_sel = prompt_seg[:, None] == seg_ids[None, :]
    prompt_len = jnp.sum(jnp.where(prompt_sel, (next_starts - doc_starts)[None, :], 0), axis=1)
    rotary_pos = places - own_start + jnp.where(prompt_seg != segment, prompt_len, 0)
    return (places, segment, prompt_seg, rotary_pos)


def rotate(values_in, rotary_pos):
    width_half = values_in.shape[-1] // 2
    frequency = jnp.exp(
        jnp.arange(width_half, dtype=jnp.float32)
        * (-2.0 * math.log(rope_base) / values_in.shape[-1])
    )
    angles = rotary_pos.astype(jnp.float32)[:, None] * frequency[None, :]
    cosine = jnp.concatenate([jnp.cos(angles), jnp.cos(angles)], axis=-1)[:, None, :]
    sine_part = jnp.concatenate([jnp.sin(angles), jnp.sin(angles)], axis=-1)[:, None, :]
    rotated = jnp.concatenate([-values_in[..., width_half:], values_in[..., :width_half]], axis=-1)
    return values_in * cosine + rotated * sine_part


def visible_mask(query_info, key_info):
    same_doc = (key_info[1][None, :] == query_info[1][:, None]) & (
        key_info[0][None, :] <= query_info[0][:, None]
    )
    from_prompt = (key_info[1][None, :] == query_info[2][:, None]) & (
        query_info[2] != query_info[1]
    )[:, None]
    return same_doc | from_prompt


def local(
    tokens,
    query_frozen_matrix,
    key_weight,
    value_frozen_matrix,
    query_down,
    query_adapter_expand,
    value_down,
    value_adapter_expand,
    block_order,
    doc_starts,
    prompt_of,
):
    tok_rows = tokens.shape[0]
    cycle_size = lax.axis_size("ctx")
    device = lax.axis_index("ctx")
    sequence_len = tok_rows * cycle_size
    block_len = tok_rows // 2
    full_tokens = lax.all_gather(tokens, "head", axis=1, tiled=True)

    def add_rows(weight_part):
        return jnp.dot(full_tokens, weight_part, preferred_element_type=jnp.float32)

    frozen_query_output = add_rows(lax.all_gather(query_frozen_matrix, "ctx", axis=0, tiled=True))
    key_base = add_rows(lax.all_gather(key_weight, "ctx", axis=0, tiled=True))
    frozen_value_output = add_rows(lax.all_gather(value_frozen_matrix, "ctx", axis=0, tiled=True))
    own_ids = device * tok_rows + jnp.arange(tok_rows, dtype=jnp.int32)
    own_info = row_meta(own_ids, block_order, doc_starts, prompt_of, block_len, sequence_len)
    local_heads = query_frozen_matrix.shape[1] // HD
    local_kv = key_weight.shape[1] // HD
    per_kv = local_heads // local_kv
    query_adapter_hidden = jnp.dot(
        full_tokens, query_down, preferred_element_type=jnp.float32
    ).astype(jnp.bfloat16)
    query_states = frozen_query_output + adapter_scaling * jnp.dot(
        query_adapter_hidden, query_adapter_expand, preferred_element_type=jnp.float32
    )
    query_states = (
        rotate(query_states.reshape(tok_rows, local_heads, HD), own_info[3]) * query_scale
    ).astype(jnp.bfloat16)
    query_heads = query_states.reshape(tok_rows, local_kv, per_kv, HD)
    key_proj = (
        rotate(key_base.reshape(tok_rows, local_kv, HD), own_info[3])
        .astype(jnp.bfloat16)
        .reshape(tok_rows, local_kv * HD)
    )
    value_adapter_hidden = jnp.dot(
        full_tokens, value_down, preferred_element_type=jnp.float32
    ).astype(jnp.bfloat16)
    value_projected = (
        frozen_value_output
        + adapter_scaling
        * jnp.dot(value_adapter_hidden, value_adapter_expand, preferred_element_type=jnp.float32)
    ).astype(jnp.bfloat16)
    pieces = (
        lax.all_gather(key_proj, "ctx", axis=0, tiled=True),
        lax.all_gather(value_projected, "ctx", axis=0, tiled=True),
    )
    key_ids = jnp.arange(pieces[0].shape[0], dtype=jnp.int32)
    key_block = pieces[0]
    value_block = pieces[1]
    key_info = row_meta(key_ids, block_order, doc_starts, prompt_of, block_len, sequence_len)
    visible = visible_mask(own_info, key_info)
    key_heads = key_block.reshape(key_block.shape[0], local_kv, HD)
    value_heads = value_block.reshape(value_block.shape[0], local_kv, HD)
    scores = jnp.einsum(
        "tkgd,skd->kgts", query_heads, key_heads, preferred_element_type=jnp.float32
    )
    capped = softcap_limit * jnp.tanh(scores / softcap_limit)
    unnorm = jnp.where(visible[None, None], jnp.exp(capped), jnp.zeros_like(capped))
    denominator = jnp.sum(unnorm, axis=-1)
    numerator = jnp.einsum(
        "kgts,skd->tkgd",
        unnorm.astype(jnp.bfloat16),
        value_heads,
        preferred_element_type=jnp.float32,
    )
    numerator, denominator = (numerator, denominator)
    attended = numerator / jnp.transpose(denominator, (2, 0, 1))[..., None]
    return attended.reshape(tok_rows, local_heads * HD).astype(jnp.bfloat16)


VMEM = pl.BlockSpec(memory_space=pltpu.VMEM)
SMEM = pl.BlockSpec(memory_space=pltpu.SMEM)
HBM = pl.BlockSpec(memory_space=pltpu.HBM)
F32, BF16 = jnp.float32, jnp.bfloat16


def in_hbm(x):
    return pltpu.with_memory_space_constraint(x, pltpu.HBM)


def call(body, outs, in_specs, flops, **kw):
    multi = isinstance(outs, (list, tuple))
    return pl.pallas_call(
        body,
        out_shape=outs,
        in_specs=in_specs,
        out_specs=[VMEM] * len(outs) if multi else VMEM,
        cost_estimate=pl.CostEstimate(flops=flops, bytes_accessed=1 << 20, transcendentals=0),
        compiler_params=pltpu.CompilerParams(vmem_limit_bytes=12 << 20),
        **kw,
    )


def place_of():
    c, h = lax.axis_index("ctx"), lax.axis_index("head")
    z = lax.shift_right_logical(h, 1)
    k = lax.bitwise_and(h, 1)
    near = lax.shift_right_logical(z, 1) == c
    return c, z, k, near


def rows_of(second):
    _, z, k, _ = place_of()
    base = lax.bitwise_and(z, 1) * 2
    if second:
        base = 2 - base
    return base + k, base + 1 - k


def dot(a, b):
    return jnp.dot(a, b, preferred_element_type=F32)


def setup_body(
    block_len, order_ref, starts_ref, prompt_ref, q_hbm, k_hbm, v_hbm, dq_hbm, dv_hbm,
    w_out, vis_out, pos_out, q_ref, k_ref, v_ref, dq_ref, dv_ref, sems,
):
    c, _, _, _ = place_of()
    half = q_ref.shape[0]
    here = pl.ds(pl.multiple_of(c * half, 128), half)
    copies = [
        pltpu.make_async_copy(src, dst, sems.at[i])
        for i, (src, dst) in enumerate(
            [
                (q_hbm, q_ref),
                (k_hbm, k_ref),
                (v_hbm, v_ref),
                (dq_hbm.at[:, here], dq_ref),
                (dv_hbm.at[:, here], dv_ref),
            ]
        )
    ]
    for copy in copies:
        copy.start()

    keys, rows = vis_out.shape
    lane = lax.broadcasted_iota(jnp.int32, (8, keys), 1)
    row = jnp.where(lane < rows, lane + c * rows, lane - c * rows)
    block = jnp.zeros_like(row)
    for i in range(1, order_ref.shape[0]):
        block += (row >= i * block_len).astype(jnp.int32)
    inside = row - block * block_len
    place = inside
    for i in range(order_ref.shape[0]):
        place = jnp.where(block == i, order_ref[i] * block_len + inside, place)
    segs = starts_ref.shape[0]
    segment, begin, prompt = jnp.zeros_like(row), jnp.zeros_like(row), jnp.zeros_like(row)
    for j in range(segs):
        reached = starts_ref[j] <= place
        segment = jnp.where(reached, j, segment)
        begin = jnp.where(reached, starts_ref[j], begin)
        prompt = jnp.where(reached, prompt_ref[j], prompt)
    length = jnp.zeros_like(row)
    for j in range(segs):
        end = starts_ref[j + 1] if j + 1 < segs else keys
        length = jnp.where(prompt == j, end - starts_ref[j], length)
    moved = place - begin + jnp.where(prompt != segment, length, 0)
    pos_out[...] = moved.astype(F32)
    key_seg = segment.astype(F32).T[:, :1]
    key_place = place.astype(F32).T[:, :1]
    mine = lambda x: x[:1, :rows].astype(F32)
    q_seg, q_place, q_prompt = mine(segment), mine(place), mine(prompt)
    q_from = jnp.where(q_prompt != q_seg, q_prompt, -1.0)
    same = (key_seg == q_seg) & (key_place <= q_place)
    vis_out[...] = jnp.where(same | (key_seg == q_from), 1.0, 0.0)

    for copy in copies:
        copy.wait()
    depth = w_out.shape[2]
    for b in range(w_out.shape[0]):
        at = 0
        span = slice(b * depth, (b + 1) * depth)
        for ref in (q_ref, k_ref, v_ref):
            w_out[b, at : at + ref.shape[1], :] = ref[span, :].T
            at += ref.shape[1]
        for ref in (dq_ref, dv_ref):
            w_out[b, at : at + ref.shape[0], :] = ref[:, span]
            at += ref.shape[0]


def first_body(w_ref, m0, m1, n0, n1, out_m, out_n):
    own, twin = rows_of(False)
    out_m[...] = dot(w_ref[own], m0[...]) + dot(w_ref[twin], m1[...])
    out_n[...] = dot(w_ref[own], n0[...]) + dot(w_ref[twin], n1[...])


def second_body(wide_q, first_sent, w_ref, x0, x1, part, eq_ref, ev_ref, keep, send):
    own, twin = rows_of(True)
    total = part[...] + dot(w_ref[own], x0[...]) + dot(w_ref[twin], x1[...])
    rank, wide_v = ev_ref.shape
    wide = send.shape[0] + first_sent
    low_q = (adapter_scaling * total[wide : wide + rank].astype(BF16)).astype(BF16)
    low_v = (adapter_scaling * total[wide + rank : wide + 2 * rank].astype(BF16)).astype(BF16)
    over = (((0,), (0,)), ((), ()))
    grow = lambda e, low: lax.dot_general(e[...], low, over, preferred_element_type=F32)
    query = total[:wide_q] + grow(eq_ref, low_q)
    key = total[wide_q : wide - wide_v]
    value = total[wide - wide_v : wide] + grow(ev_ref, low_v)
    keep[:wide_q] = query
    keep[wide_q : wide - wide_v] = key
    keep[wide - wide_v :] = value
    if first_sent == 0:
        send[:wide_q] = query.astype(BF16)
    send[wide_q - first_sent : wide - wide_v - first_sent] = key.astype(BF16)
    send[wide - wide_v - first_sent :] = value.astype(BF16)


def pick_body(a_ref, b_ref, out_ref):
    near = place_of()[3]

    @pl.when(near)
    def _():
        out_ref[...] = a_ref[...]

    @pl.when(jnp.logical_not(near))
    def _():
        out_ref[...] = b_ref[...]


def turn(x, cos, sin):
    half = x.shape[0] // 2
    a, b = x[:half], x[half:]
    return jnp.concatenate([a * cos - b * sin, b * cos + a * sin], axis=0)


def weigh(keys, queries, values, visible, heads):
    rows = visible.shape[1]
    scores = dot(keys.T, queries)
    weights = jnp.exp(softcap_limit * jnp.tanh(scores / softcap_limit))
    sums, products = [], []
    for h in range(heads):
        w = weights[:, h * rows : (h + 1) * rows] * visible
        sums.append(jnp.sum(w, axis=0, keepdims=True))
        products.append(dot(values, w.astype(BF16)))
    return jnp.concatenate(sums, axis=1), jnp.concatenate(products, axis=1)


def near_body(heads, mine, mine_in, cos_ref, sin_ref, vis_ref, q_out, sum_out, num_out):
    rows = mine.shape[1]
    wide_q = heads * HD
    cos, sin = cos_ref[:, :rows], sin_ref[:, :rows]
    total = mine[...] + mine_in[...].astype(F32)
    queries = jnp.concatenate(
        [
            (turn(total[h * HD : (h + 1) * HD], cos, sin) * query_scale).astype(BF16)
            for h in range(heads)
        ],
        axis=1,
    )
    keys = turn(total[wide_q : wide_q + HD], cos, sin).astype(BF16)
    values = total[wide_q + HD :].astype(BF16)
    q_out[...] = queries
    sums, num_out[...] = weigh(keys, queries, values, vis_ref[:rows, :], heads)
    sum_out[...] = jnp.broadcast_to(sums, sum_out.shape)


def far_body(heads, other, other_in, q_ref, sum_ref, num_ref, cos_ref, sin_ref, vis_ref, out_ref):
    rows = other.shape[1]
    rest = other[heads * HD :] + other_in[...].astype(F32)
    keys = turn(rest[:HD], cos_ref[:, rows:], sin_ref[:, rows:]).astype(BF16)
    sums, products = weigh(
        keys, q_ref[...], rest[HD:].astype(BF16), vis_ref[rows:, :], heads
    )
    done = (num_ref[...] + products) / (sum_ref[:1, :] + sums)
    for h in range(heads):
        out_ref[:, h * HD : (h + 1) * HD] = done[:, h * rows : (h + 1) * rows].T.astype(BF16)


def local_fast(
    tokens,
    query_frozen_matrix,
    key_weight,
    value_frozen_matrix,
    query_down,
    query_adapter_expand,
    value_down,
    value_adapter_expand,
    block_order,
    doc_starts,
    prompt_of,
):
    rows, depth = tokens.shape
    chips = lax.axis_size("head") // 2
    both = ("ctx", "head")

    def at(ci, zi, ki):
        return ci * chips * 2 + zi * 2 + ki

    q1_pairs, q2_pairs, z_pairs, zf_pairs = [], [], [], []
    for ci in range(2):
        for zi in range(chips):
            for ki in range(2):
                me = at(ci, zi, ki)
                z_pairs.append((me, at(ci, zi ^ 1, ki)))
                if zi // 2 == ci:
                    q1_pairs.append((me, at(ci, zi ^ 2, ki)))
                    q2_pairs.append((me, at(ci, zi ^ 1, ki)))
                else:
                    q1_pairs.append((me, at(1 - ci, zi, ki)))
                    q2_pairs.append((me, at(1 - ci, zi ^ 2, ki)))
                    zf_pairs.append((me, at(ci, zi ^ 1, ki)))
    core = [(i, i ^ 1) for i in range(chips * 2)]
    swap = [(0, 1), (1, 0)]

    def send(x, pairs, axes=both):
        return lax.ppermute(x, axes, pairs)

    def twin(x):
        return send(x, core, "head")

    own = tokens.T
    q1 = send(own, q1_pairs)
    q2 = send(own, q2_pairs)

    wide_q, wide_kv = query_frozen_matrix.shape[1], key_weight.shape[1]
    wide = wide_q + 2 * wide_kv
    rank = query_down.shape[1]
    half = query_frozen_matrix.shape[0]
    keys = 2 * rows

    def setup(*refs):
        setup_body(rows // 2, *refs)

    weights, visible, moved = pl.pallas_call(
        setup,
        out_shape=[
            jax.ShapeDtypeStruct((half // depth, wide + 2 * rank, depth), BF16),
            jax.ShapeDtypeStruct((keys, rows), F32),
            jax.ShapeDtypeStruct((8, keys), F32),
        ],
        in_specs=[SMEM] * 3 + [HBM] * 5,
        out_specs=[VMEM] * 3,
        scratch_shapes=[
            pltpu.VMEM((half, wide_q), BF16),
            pltpu.VMEM((half, wide_kv), BF16),
            pltpu.VMEM((half, wide_kv), BF16),
            pltpu.VMEM((rank, half), BF16),
            pltpu.VMEM((rank, half), BF16),
            pltpu.SemaphoreType.DMA((5,)),
        ],
        cost_estimate=pl.CostEstimate(flops=10**9, bytes_accessed=1 << 20, transcendentals=0),
        compiler_params=pltpu.CompilerParams(vmem_limit_bytes=12 << 20),
    )(
        block_order,
        doc_starts,
        prompt_of,
        in_hbm(query_frozen_matrix),
        in_hbm(key_weight),
        in_hbm(value_frozen_matrix),
        in_hbm(query_down.T),
        in_hbm(value_down.T),
    )

    def pick(a, b):
        out = jax.ShapeDtypeStruct(a.shape, a.dtype)
        return call(pick_body, out, [VMEM, VMEM], 10**7)(a, b)

    other_a = pick(q1, q2)
    other_b = send(other_a, z_pairs)
    late = send(q1, zf_pairs)
    mine_a = pick(own, q1)
    mine_b = pick(q2, late)

    whole = jax.ShapeDtypeStruct((wide + 2 * rank, rows), F32)
    kept = jax.ShapeDtypeStruct((wide, rows), F32)
    other_twin, mine_twin = twin(other_a), twin(mine_a)
    part_m, part_n = call(first_body, [whole, whole], [VMEM] * 5, 10**9)(
        weights, other_a, other_twin, mine_a, mine_twin
    )

    def second(x, part, first_sent):
        def body(*refs):
            second_body(wide_q, first_sent, *refs)

        outs = [kept, jax.ShapeDtypeStruct((wide - first_sent, rows), BF16)]
        other = twin(x)
        return call(body, outs, [VMEM] * 6, 5 * 10**8)(
            weights, x, other, part, query_adapter_expand, value_adapter_expand
        )

    other_keep, other_send = second(other_b, part_m, 0)
    mine_in = send(other_send, swap, "ctx")
    frequency = jnp.exp(
        jnp.arange(HD // 2, dtype=F32) * (-2.0 * math.log(rope_base) / HD)
    )
    angles = frequency[:, None] * moved[:1]
    cos, sin = jnp.cos(angles), jnp.sin(angles)
    mine_keep, mine_send = second(mine_b, part_n, wide_q)
    other_in = send(mine_send, swap, "ctx")

    heads = wide_q // HD

    def near_keys(*refs):
        near_body(heads, *refs)

    def far_keys(*refs):
        far_body(heads, *refs)

    outs = [
        jax.ShapeDtypeStruct((HD, heads * rows), BF16),
        jax.ShapeDtypeStruct((8, heads * rows), F32),
        jax.ShapeDtypeStruct((HD, heads * rows), F32),
    ]
    queries, sums, products = call(near_keys, outs, [VMEM] * 5, 10**9)(
        mine_keep, mine_in, cos, sin, visible
    )
    return call(far_keys, jax.ShapeDtypeStruct((rows, wide_q), BF16), [VMEM] * 8, 10**9)(
        other_keep, other_in, queries, sums, products, cos, sin, visible
    )


def solution(mesh):
    in_specs = (
        P(("tenant", "ctx"), "head"),
        P("ctx", "head"),
        P("ctx", "head"),
        P("ctx", "head"),
        P("tenant", None),
        P("tenant", "head"),
        P("tenant", None),
        P("tenant", "head"),
        P("tenant"),
        P("tenant"),
        P("tenant"),
    )
    out_specs = P(("tenant", "ctx"), "head")
    fits = mesh.shape["ctx"] == 2 and mesh.shape["head"] == 8

    def body(*args):
        if not fits:
            return local(*args)
        return local_fast(*args)

    return jax.shard_map(
        body, mesh=mesh, in_specs=in_specs, out_specs=out_specs, check_vma=False
    )
```
